8 devices in a mesh: rep: 1 (over z), dp: 2 (over y), ad: 4 (over x, core).
Axes of the slice: x: 2, y: 2, z: 1, core: 2. Of those that a mesh axis runs over, the one named last changes fastest.
Arguments:
- x_rows: bfloat16 [16384, 3584], P(('rep', 'dp', 'ad'))
- adapter_id: int32 [16384], P(('rep', 'dp', 'ad'))
- w_gate: bfloat16 [3584, 18944], replicated
- w_up: bfloat16 [3584, 18944], replicated
- w_down: bfloat16 [18944, 3584], replicated
- a_gate: bfloat16 [8, 3584, 64], P('ad')
- b_gate: bfloat16 [8, 64, 18944], P('ad')
- a_up: bfloat16 [8, 3584, 64], P('ad')
- b_up: bfloat16 [8, 64, 18944], P('ad')
- a_down: bfloat16 [8, 18944, 64], P('ad')
- b_down: bfloat16 [8, 64, 3584], P('ad')
Outputs:
- output: bfloat16 [16384, 3584], P(('rep', 'dp', 'ad'))
All inputs are finite; a program needn't handle non-finite values.
Results may differ from the reference program's by a relative error of at most 0.00179.
Values are sent between devices in bfloat16 or wider.
A program may use at most 1.75 GiB of HBM per device.

```python
import jax
import jax.numpy as jnp
from jax import lax

D_MODEL = 3584
D_FF = 18944
RANK = 64
LORA_ALPHA = 32
TOKENS_DEV = 2048
GROUP = 4
REPLICAS = 2
ADAPTERS = 8
ROW_BLOCK = 32
SOURCES = REPLICAS * GROUP
TOKENS = SOURCES * TOKENS_DEV
ADAPT_LOCAL = ADAPTERS // GROUP
CAPACITY = (TOKENS_DEV // GROUP) * min(4, max(1, GROUP // 2))


def draw_adapter_ids(key_ids):
    key_hot, key_off, key_perm, key_tok = jax.random.split(key_ids, 4)
    hot_base = jax.random.randint(key_hot, (), 0, GROUP)
    offset = jax.random.randint(key_off, (), 0, ADAPT_LOCAL)
    labels = jax.random.permutation(key_perm, ADAPT_LOCAL)
    source = jnp.arange(SOURCES)
    hot_owner = (hot_base + source // GROUP) % GROUP
    distance = (jnp.arange(GROUP)[None, :] - hot_owner[:, None]) % GROUP
    rest = TOKENS_DEV - CAPACITY
    cold_base = rest // (GROUP - 1)
    cold_extra = rest % (GROUP - 1)
    counts = jnp.where(distance == 0, CAPACITY, cold_base + (distance - 1 < cold_extra).astype(jnp.int32))
    owner_sorted = jax.vmap(lambda count_row: jnp.repeat(jnp.arange(GROUP), count_row, total_repeat_length=TOKENS_DEV))(counts)
    starts = jnp.cumsum(counts, axis=1) - counts
    within = jnp.arange(TOKENS_DEV)[None, :] - jnp.take_along_axis(starts, owner_sorted, axis=1)
    spread = within * SOURCES + source[:, None] + offset
    ids_sorted = owner_sorted * ADAPT_LOCAL + labels[spread % ADAPT_LOCAL]
    orders = jax.vmap(lambda sub_key: jax.random.permutation(sub_key, TOKENS_DEV))(jax.random.split(key_tok, SOURCES))
    return jnp.take_along_axis(ids_sorted, orders, axis=1).reshape(-1).astype(jnp.int32)


def setup_inputs(seed: int = 0, part: int = 0) -> dict:
    key_part = jax.random.fold_in(jax.random.key(seed), part)
    key_x, key_ids = jax.random.split(key_part)
    keys = jax.random.split(jax.random.key(seed + 1), 9)
    scale = LORA_ALPHA / RANK
    up_std = 0.4 / (scale * RANK ** 0.5)
    down_std = 0.5 / (scale * RANK ** 0.5)

    def normal(sub_key, shape, std_dev):
        return (jax.random.normal(sub_key, shape, jnp.float32) * std_dev).astype(jnp.bfloat16)

    return {
        "x_rows": normal(key_x, (TOKENS, D_MODEL), 1.0),
        "adapter_id": draw_adapter_ids(key_ids),
        "w_gate": normal(keys[0], (D_MODEL, D_FF), D_MODEL ** -0.5),
        "w_up": normal(keys[1], (D_MODEL, D_FF), D_MODEL ** -0.5),
        "w_down": normal(keys[2], (D_FF, D_MODEL), D_FF ** -0.5),
        "a_gate": normal(keys[3], (ADAPTERS, D_MODEL, RANK), D_MODEL ** -0.5),
        "b_gate": normal(keys[4], (ADAPTERS, RANK, D_FF), up_std),
        "a_up": normal(keys[5], (ADAPTERS, D_MODEL, RANK), D_MODEL ** -0.5),
        "b_up": normal(keys[6], (ADAPTERS, RANK, D_FF), up_std),
        "a_down": normal(keys[7], (ADAPTERS, D_FF, RANK), D_FF ** -0.5),
        "b_down": normal(keys[8], (ADAPTERS, RANK, D_MODEL), down_std),
    }


def reference(x_rows, adapter_id, w_gate, w_up, w_down, a_gate, b_gate, a_up, b_up, a_down, b_down):
    scale = LORA_ALPHA / RANK
    n_blocks = TOKENS // ROW_BLOCK

    def low_rank(rows_in, block_ids, a_mat, b_mat):
        a_sel = jnp.take(a_mat, block_ids, axis=0).astype(jnp.float32)
        low_proj = jnp.einsum("tk,tkr->tr", rows_in.astype(jnp.float32), a_sel).astype(jnp.bfloat16)
        b_sel = jnp.take(b_mat, block_ids, axis=0).astype(jnp.float32)
        wide_proj = jnp.einsum("tr,trn->tn", low_proj.astype(jnp.float32), b_sel)
        return (scale * wide_proj).astype(jnp.bfloat16).astype(jnp.float32)

    def one_block(block):
        x_blk, block_ids = block
        gate_pre = jnp.dot(x_blk, w_gate, preferred_element_type=jnp.float32) + low_rank(x_blk, block_ids, a_gate, b_gate)
        up_proj = jnp.dot(x_blk, w_up, preferred_element_type=jnp.float32) + low_rank(x_blk, block_ids, a_up, b_up)
        hidden = (jax.nn.silu(gate_pre) * up_proj).astype(jnp.bfloat16)
        down_proj = jnp.dot(hidden, w_down, preferred_element_type=jnp.float32) + low_rank(hidden, block_ids, a_down, b_down)
        return (x_blk.astype(jnp.float32) + down_proj).astype(jnp.bfloat16)

    result = lax.map(one_block, (x_rows.reshape(n_blocks, ROW_BLOCK, D_MODEL), adapter_id.reshape(n_blocks, ROW_BLOCK)))
    return result.reshape(TOKENS, D_MODEL)
```

```python
import functools

import jax
import jax.numpy as jnp
from jax import lax
from jax.experimental import pallas as pl
from jax.experimental.pallas import tpu as pltpu
from jax.sharding import PartitionSpec as P

LORA_ALPHA = 32
BLOCK = 512
TILE = 512
HALF = 1024
RAW_BLOCKS = 3
FIRST_BLOCKS = 8
VMEM_BYTES = 66_000_000
F32 = jnp.float32
BF16 = jnp.bfloat16


def dot(a, b):
    return jnp.dot(a, b, preferred_element_type=F32)


def dot_t(a, b):
    return lax.dot_general(a, b, (((1,), (1,)), ((), ())), preferred_element_type=F32)


def rounded(scale, wide):
    return (scale * wide).astype(BF16).astype(F32)


def activation(scale, gate, up, wide_gate, wide_up):
    gate = gate + rounded(scale, wide_gate)
    up = up + rounded(scale, wide_up)
    return (gate * jax.nn.sigmoid(gate) * up).astype(BF16)


def cost(flops, bytes_accessed):
    return pl.CostEstimate(flops=int(flops), bytes_accessed=int(bytes_accessed), transcendentals=0)


def params(semantics):
    return pltpu.CompilerParams(dimension_semantics=semantics, vmem_limit_bytes=VMEM_BYTES)


def base_kernel(x_ref, wg_ref, wu_ref, gate_ref, up_ref):
    def tile(t, _):
        rows = pl.ds(pl.multiple_of(t * TILE, TILE), TILE)
        gate_ref[rows, :] = dot(x_ref[rows, :], wg_ref[...])
        up_ref[rows, :] = dot(x_ref[rows, :], wu_ref[...])
        return 0

    lax.fori_loop(0, x_ref.shape[0] // TILE, tile, 0)


def base_products(x_rows, w_gate, w_up, n_blocks):
    n_rows, d_model = x_rows.shape
    raw = jax.ShapeDtypeStruct((n_rows, n_blocks * BLOCK), F32)
    whole = pl.BlockSpec((n_rows, d_model), lambda j: (0, 0), pipeline_mode=pl.Buffered(1))
    weight = pl.BlockSpec((d_model, BLOCK), lambda j: (0, j))
    block = pl.BlockSpec((n_rows, BLOCK), lambda j: (0, j))
    return pl.pallas_call(
        base_kernel, grid=(n_blocks,), out_shape=(raw, raw), in_specs=[whole, weight, weight],
        out_specs=(block, block), compiler_params=params(("arbitrary",)), name="base_products",
        cost_estimate=cost(4 * n_rows * d_model * n_blocks * BLOCK, 4 * d_model * n_blocks * BLOCK),
    )(x_rows, w_gate, w_up)


def gate_up_kernel(scale, first, aliased, x_ref, wg_ref, wu_ref, lg_ref, lu_ref, bg_ref, bu_ref, *rest):
    if aliased:
        rest = rest[1:]
    h_ref, h_buf, ga, ua, wga, wua, gb, ub, wgb, wub, sems = rest
    j, n_steps = pl.program_id(0), pl.num_programs(0)
    n_tiles = x_ref.shape[0] // TILE
    sets = ((ga, ua, wga, wua), (gb, ub, wgb, wub))

    def copy_out(step):
        cols = pl.ds(pl.multiple_of((first + step) * BLOCK, BLOCK), BLOCK)
        return pltpu.make_async_copy(h_buf.at[step % 2], h_ref.at[:, cols], sems.at[step % 2])

    def products(t, dst):
        rows = pl.ds(pl.multiple_of(t * TILE, TILE), TILE)
        x_t = x_ref[rows, :]
        dst[0][...] = dot(x_t, wg_ref[...])
        dst[1][...] = dot(x_t, wu_ref[...])
        dst[2][...] = dot(lg_ref[rows, :], bg_ref[...])
        dst[3][...] = dot(lu_ref[rows, :], bu_ref[...])

    def finish(src, slot, t):
        chunk = 32
        for r in range(0, TILE, chunk):
            part = pl.ds(r, chunk)
            rows = pl.ds(pl.multiple_of(t * TILE + r, chunk), chunk)
            h_buf[slot, rows, :] = activation(scale, *(s[part, :] for s in src))

    @pl.when(j >= 2)
    def _():
        copy_out(j - 2).wait()

    slot, other = j % 2, (j + 1) % 2
    products(0, sets[0])
    finish(sets[1], other, n_tiles - 1)

    @pl.when(j >= 1)
    def _():
        copy_out(j - 1).start()

    def pair(p, _):
        products(2 * p + 1, sets[1])
        finish(sets[0], slot, 2 * p)
        products(2 * p + 2, sets[0])
        finish(sets[1], slot, 2 * p + 1)
        return 0

    lax.fori_loop(0, n_tiles // 2 - 1, pair, 0)
    products(n_tiles - 1, sets[1])
    finish(sets[0], slot, n_tiles - 2)

    @pl.when(j == n_steps - 1)
    def _():
        finish(sets[1], slot, n_tiles - 1)
        copy_out(j).start()

        @pl.when(j >= 1)
        def _():
            copy_out(j - 1).wait()

        copy_out(j).wait()


def gate_up(scale, x_rows, w_gate, w_up, low, b_mat, first, n_blocks, gate_at, up_at, hidden):
    n_rows, d_model = x_rows.shape
    d_ff, rank = w_gate.shape[1], b_mat.shape[0]
    once = pl.Buffered(1)
    weight = pl.BlockSpec((d_model, BLOCK), lambda j: (0, first + j))
    whole = pl.BlockSpec((n_rows, d_model), lambda j: (0, 0), pipeline_mode=once)
    narrow = pl.BlockSpec((n_rows, rank), lambda j: (0, 0), pipeline_mode=once)
    in_specs = [whole, weight, weight, narrow, narrow,
                pl.BlockSpec((rank, BLOCK), lambda j: (0, gate_at + j)),
                pl.BlockSpec((rank, BLOCK), lambda j: (0, up_at + j))]
    args = [x_rows, w_gate, w_up, low[0], low[1], b_mat, b_mat]
    aliases = {}
    if hidden is not None:
        in_specs.append(pl.BlockSpec(memory_space=pl.ANY))
        aliases = {len(args): 0}
        args.append(hidden)
    width = n_blocks * BLOCK
    return pl.pallas_call(
        functools.partial(gate_up_kernel, scale, first, hidden is not None), grid=(n_blocks,),
        out_shape=jax.ShapeDtypeStruct((n_rows, d_ff), BF16), in_specs=in_specs,
        out_specs=pl.BlockSpec(memory_space=pl.ANY),
        scratch_shapes=[pltpu.VMEM((2, n_rows, BLOCK), BF16)] + [pltpu.VMEM((TILE, BLOCK), F32)] * 8
        + [pltpu.SemaphoreType.DMA((2,))],
        input_output_aliases=aliases, compiler_params=params(("arbitrary",)), name="gate_up",
        cost_estimate=cost(4 * n_rows * (d_model + rank) * width, 4 * d_model * width),
    )(*args)


def finish_kernel(scale, gate_ref, up_ref, lg_ref, lu_ref, bg_ref, bu_ref, hidden_ref, h_ref):
    def tile(t, _):
        rows = pl.ds(pl.multiple_of(t * TILE, TILE), TILE)
        h_ref[rows, :] = activation(scale, gate_ref[rows, :], up_ref[rows, :],
                                    dot(lg_ref[rows, :], bg_ref[...]), dot(lu_ref[rows, :], bu_ref[...]))
        return 0

    lax.fori_loop(0, gate_ref.shape[0] // TILE, tile, 0)


def finish_raw(scale, raw, low, b_mat, gate_at, up_at, hidden):
    n_rows, width = raw[0].shape
    rank = b_mat.shape[0]
    block = pl.BlockSpec((n_rows, BLOCK), lambda j: (0, j))
    narrow = pl.BlockSpec((n_rows, rank), lambda j: (0, 0), pipeline_mode=pl.Buffered(1))
    return pl.pallas_call(
        functools.partial(finish_kernel, scale), grid=(width // BLOCK,),
        out_shape=jax.ShapeDtypeStruct(hidden.shape, BF16),
        in_specs=[block, block, narrow, narrow,
                  pl.BlockSpec((rank, BLOCK), lambda j: (0, gate_at + j)),
                  pl.BlockSpec((rank, BLOCK), lambda j: (0, up_at + j)),
                  pl.BlockSpec(memory_space=pl.ANY)],
        out_specs=block, input_output_aliases={6: 0}, compiler_params=params(("arbitrary",)), name="finish_raw",
        cost_estimate=cost(4 * n_rows * rank * width, 10 * n_rows * width),
    )(raw[0], raw[1], low[0], low[1], b_mat, b_mat, hidden)


def down_kernel(scale, adapter_rank, h_ref, wd_ref, a_ref, b_ref, x_ref, id_ref, out_ref, acc, low_acc):
    k, n_steps = pl.program_id(1), pl.num_programs(1)
    d_model = wd_ref.shape[1]
    tile = 512

    @pl.when(k == 0)
    def _():
        acc[...] = jnp.zeros_like(acc)
        low_acc[...] = jnp.zeros_like(low_acc)

    for m in range(0, HALF, tile):
        rows = pl.ds(m, tile)
        for n in range(0, d_model, tile):
            cols = pl.ds(n, tile)
            acc[rows, cols] += dot(h_ref[rows, :], wd_ref[:, cols])
        low_acc[rows, :] += dot_t(h_ref[rows, :], a_ref[...])

    @pl.when(k == n_steps - 1)
    def _():
        column = lax.broadcasted_iota(jnp.int32, low_acc.shape, 1) // adapter_rank
        low = jnp.where(column == id_ref[...], low_acc[...], 0.0).astype(BF16)
        low_acc[...] = low.astype(F32)

        def part(m, _):
            rows = pl.ds(pl.multiple_of(m * TILE, TILE), TILE)
            low = low_acc[rows, :].astype(BF16)
            for n in range(0, d_model, tile):
                cols = pl.ds(n, tile)
                total = acc[rows, cols] + rounded(scale, dot(low, b_ref[:, cols]))
                out_ref[rows, cols] = (x_ref[rows, cols].astype(F32) + total).astype(BF16)
            return 0

        lax.fori_loop(0, HALF // TILE, part, 0)


def down(scale, adapter_rank, hidden, w_down, adapters, x_rows, slots):
    n_rows, d_model = x_rows.shape
    d_ff, rank = w_down.shape[0], adapters.shape[0]
    once = pl.Buffered(1)
    row_block = pl.BlockSpec((HALF, d_model), lambda i, k: (i, 0), pipeline_mode=once)
    return pl.pallas_call(
        functools.partial(down_kernel, scale, adapter_rank), grid=(n_rows // HALF, d_ff // BLOCK),
        out_shape=jax.ShapeDtypeStruct((n_rows, d_model), BF16),
        in_specs=[pl.BlockSpec((HALF, BLOCK), lambda i, k: (i, k)),
                  pl.BlockSpec((BLOCK, d_model), lambda i, k: (k, 0)),
                  pl.BlockSpec((rank, BLOCK), lambda i, k: (0, d_model // BLOCK + k)),
                  pl.BlockSpec((rank, d_model), lambda i, k: (0, 0), pipeline_mode=once),
                  row_block,
                  pl.BlockSpec((HALF, 1), lambda i, k: (i, 0), pipeline_mode=once)],
        out_specs=pl.BlockSpec((HALF, d_model), lambda i, k: (i, 0)),
        scratch_shapes=[pltpu.VMEM((HALF, d_model), F32), pltpu.VMEM((HALF, rank), F32)],
        compiler_params=params(("arbitrary", "arbitrary")), name="down",
        cost_estimate=cost(2 * n_rows * d_ff * (d_model + rank), 4 * d_ff * d_model),
    )(hidden, w_down, adapters, adapters, x_rows, slots)


def solution(mesh):
    n_dp, n_ad = mesh.shape["dp"], mesh.shape["ad"]
    row_spec = P(("rep", "dp", "ad"), None)
    owned = P("ad", None, None)

    def local_step(x_rows, adapter_id, w_gate, w_up, w_down, a_gate, b_gate, a_up, b_up, a_down, b_down):
        n_local, d_model, rank = a_gate.shape
        d_ff = w_gate.shape[1]
        scale = LORA_ALPHA / rank
        share = n_local // n_dp
        dp = lax.axis_index("dp")

        def mine(mat):
            return lax.dynamic_slice_in_dim(mat, dp * share, share, axis=0)

        def flat(mat):
            return mat.reshape(share * rank, mat.shape[2])

        def gather(parts):
            return lax.all_gather(jnp.concatenate(parts, axis=1), ("dp", "ad"), axis=0, tiled=True)

        owner, local = adapter_id // n_local, adapter_id % n_local
        slots = ((local // share) * n_ad + owner) * share + local % share

        n_all = d_ff // BLOCK
        n_raw, n_first = RAW_BLOCKS, FIRST_BLOCKS
        n_last = n_all - n_raw - n_first
        cut0, cut1 = n_raw * BLOCK, (n_raw + n_first) * BLOCK
        at_gate, at_up, at_down = (flat(jnp.swapaxes(mine(m), 1, 2)) for m in (a_gate, a_up, a_down))
        bt_gate, bt_up, bt_down = (flat(mine(m)) for m in (b_gate, b_up, b_down))

        a_all = gather([at_gate, at_up])
        b_first = gather([bt_gate[:, cut0:cut1], bt_up[:, cut0:cut1]])
        b_last = gather([bt_gate[:, cut1:], bt_gate[:, :cut0], bt_up[:, cut1:], bt_up[:, :cut0]])
        down_all = gather([bt_down, at_down])

        raw = base_products(x_rows, w_gate, w_up, n_raw)
        column = lax.broadcasted_iota(jnp.int32, (x_rows.shape[0], a_all.shape[0]), 1) // rank
        keep = column == slots[:, None]
        low = [jnp.where(keep, dot_t(x_rows, a), 0.0).astype(BF16) for a in (a_all[:, :d_model], a_all[:, d_model:])]
        hidden = gate_up(scale, x_rows, w_gate, w_up, low, b_first, n_raw, n_first, 0, n_first, None)
        hidden = gate_up(scale, x_rows, w_gate, w_up, low, b_last, n_raw + n_first, n_last, 0, n_last + n_raw, hidden)
        hidden = finish_raw(scale, raw, low, b_last, n_last, 2 * n_last + n_raw, hidden)
        return down(scale, rank, hidden, w_down, down_all, x_rows, slots[:, None])

    return jax.shard_map(local_step, mesh=mesh,
                         in_specs=(row_spec, P(("rep", "dp", "ad")), P(), P(), P(), owned, owned, owned, owned, owned, owned),
                         out_specs=row_spec, check_vma=False)
```
